32 devices in a mesh: rep: 4 (over z), fsdp: 2 (over x), tp: 4 (over y, core).
Axes of the slice: x: 2, y: 2, z: 4, core: 2. Of those that a mesh axis runs over, the one named last changes fastest.
Arguments:
- gate_pre: bfloat16 [1024, 14848], P(('rep', 'fsdp'), 'tp'), may hold values from -6 to 6
- up_pre: bfloat16 [1024, 14848], P(('rep', 'fsdp'), 'tp'), may hold values from -30 to 30
- out_grad: bfloat16 [1024, 4096], P(('rep', 'fsdp')), may hold values from -30 to 30
Outputs:
- down_grad: bfloat16 [4096, 14848], P('fsdp', 'tp')
The draws below stay inside these ranges and needn't reach their ends.
All inputs are finite; a program needn't handle non-finite values.
Results may differ from the reference program's by a relative error of at most 0.02.
Values may be sent and summed in bfloat16 or wider, within the bound.
A program may use at most 128 MiB of HBM per device.

```python
import jax
import jax.numpy as jnp
from jax import lax

D = 4096
FF = 14848
TOK_DEV = 128
TOKENS = 1024
N_REP = 4
N_FSDP = 2


def draw_up_pre(key, part):
    subkeys = jax.random.split(jax.random.fold_in(key, 11), 2)
    position = jnp.arange(FF, dtype=jnp.float32) / FF
    roughness = jax.random.uniform(subkeys[1], (FF,), jnp.float32, 1.0, 2.0)
    entries = jnp.clip(jax.random.normal(subkeys[0], (TOKENS, FF), jnp.float32), -5.0, 5.0)
    column_scale = 3.0 ** position * roughness / 3.0
    return (entries * column_scale[None, :]).astype(jnp.bfloat16)


def draw_out_grad(key, part):
    subkeys = jax.random.split(jax.random.fold_in(key, 23), 2)
    position = jnp.arange(D, dtype=jnp.float32) / D
    roughness = jax.random.uniform(subkeys[1], (D,), jnp.float32, 1.0, 2.0)
    entries = jnp.clip(jax.random.normal(subkeys[0], (TOKENS, D), jnp.float32), -5.0, 5.0)
    column_scale = 3.0 ** position * roughness / 3.0
    return (entries * column_scale[None, :]).astype(jnp.bfloat16)


def levels(stream_key, shape, cuts, least, top_value):
    def one(axis_at, parts):
        steps = jax.random.uniform(jax.random.fold_in(jax.random.fold_in(stream_key, 6), axis_at), (parts,), jnp.float32, least / len(cuts), top_value / len(cuts))
        return jnp.repeat(jnp.exp(steps), shape[axis_at] // parts).reshape((-1,) + (1,) * (len(shape) - axis_at - 1))

    gain = one(*cuts[0])
    for cut in cuts[1:]:
        gain = gain * one(*cut)
    return gain


def centred(rng, shape, deviation, limit, pieces=(), held_as=jnp.bfloat16):
    loudness = levels(rng, shape, pieces, -0.22, 0.18) if pieces else 1.0
    result = jax.random.normal(rng, shape, jnp.float32) * deviation * loudness
    return jnp.minimum(jnp.maximum(result, -limit), limit).astype(held_as)


def setup_inputs(seed: int = 0) -> dict:
    arg_keys = jax.random.split(jax.random.key(seed), 4)
    gate_pre = centred(arg_keys[0], (TOKENS, FF), 1.0, 6.0, ((0, 8), (1, 4)))
    up_pre = draw_up_pre(jax.random.fold_in(arg_keys[3], 71), 0)
    out_grad = draw_out_grad(jax.random.fold_in(arg_keys[3], 71), 0)
    return {"gate_pre": gate_pre, "up_pre": up_pre, "out_grad": out_grad}


def reference(gate_pre, up_pre, out_grad):
    hidden = (jax.nn.silu(gate_pre.astype(jnp.float32)) * up_pre.astype(jnp.float32)).astype(jnp.bfloat16)
    hidden_blocks = hidden.reshape(N_REP, N_FSDP, TOK_DEV, FF)
    grad_blocks = out_grad.reshape(N_REP, N_FSDP, TOK_DEV, D)

    def inner_add(running, paired):
        grad_rows, hidden_rows = paired
        partial_term = jnp.dot(grad_rows.T, hidden_rows, preferred_element_type=jnp.float32)
        return (running + partial_term.astype(jnp.bfloat16).astype(jnp.float32), None)

    def outer_add(running, paired):
        starting = jnp.zeros((D, FF), jnp.float32)
        replica_part, unused = lax.scan(inner_add, starting, paired)
        return (running + replica_part.astype(jnp.bfloat16).astype(jnp.float32), None)
    summed, unused = lax.scan(outer_add, jnp.zeros((D, FF), jnp.float32), (grad_blocks, hidden_blocks))
    square_total = jnp.sum(summed * summed)
    factor = 1.0 / jnp.sqrt(square_total / (D * FF) + 1e-06)
    return (summed * factor).astype(jnp.bfloat16)
```

```python
import jax
import jax.numpy as jnp
from jax import lax
from jax.sharding import PartitionSpec as P


def on_device(gate_pre, up_pre, out_grad):
    hidden = (jax.nn.silu(gate_pre.astype(jnp.float32)) * up_pre.astype(jnp.float32)).astype(
        jnp.bfloat16
    )
    spread = lax.all_to_all(out_grad, "fsdp", split_axis=1, concat_axis=0, tiled=True)
    grad_rows = lax.all_gather(spread, "rep", axis=0, tiled=True)
    hidden_rows = lax.all_gather(hidden, ("rep", "fsdp"), axis=0, tiled=True)
    summed = lax.dot_general(
        grad_rows, hidden_rows, (((0,), (0,)), ((), ())), preferred_element_type=jnp.float32
    )
    square_total = lax.psum(jnp.sum(summed * summed), ("fsdp", "tp"))
    entry_count = summed.shape[0] * lax.axis_size("fsdp") * summed.shape[1] * lax.axis_size("tp")
    factor = 1.0 / jnp.sqrt(square_total / entry_count + 1e-06)
    return (summed * factor).astype(jnp.bfloat16)


def solution(mesh):
    return jax.shard_map(
        on_device,
        mesh=mesh,
        in_specs=(P(("rep", "fsdp"), "tp"), P(("rep", "fsdp"), "tp"), P(("rep", "fsdp"), None)),
        out_specs=P("fsdp", "tp"),
        check_vma=False,
    )
```

```python
import functools

import jax
import jax.numpy as jnp
from jax import lax
from jax.experimental import pallas as pl
from jax.experimental.pallas import tpu as pltpu
from jax.sharding import PartitionSpec as P

MESH = pl.DeviceIdType.MESH
LANES = 128
VMEM_LIMIT = 60 * 1024 * 1024


def column_chunks(columns):
    chunks, start = [], 0
    for tiles in (6, 4, 2, 1):
        while columns - start >= tiles * LANES:
            chunks.append((start, tiles * LANES))
            start += tiles * LANES
    return chunks


def gather_multiply(
    n_rep, n_tp, hidden_ref, grad_ref, out_ref, square_ref,
    held, grads, turned, staged,
    local_sem, gx_send, gx_recv, gz_send, gz_recv, gt_send, gt_recv,
    hz_send, hz_recv, hx_send, hx_recv, out_sem,
):
    rep = lax.axis_index("rep")
    fsdp = lax.axis_index("fsdp")
    tp = lax.axis_index("tp")
    rows, columns = hidden_ref.shape
    half = grads.shape[1]
    quarter = half // n_tp
    chunks = column_chunks(columns)
    pair = 2 * rows
    my_slot = rep * 2 + fsdp
    my_rows = pl.ds(pl.multiple_of(my_slot * rows, rows), rows)
    other_rows = pl.ds(pl.multiple_of((rep * 2 + 1 - fsdp) * rows, rows), rows)
    across = {"fsdp": 1 - fsdp}
    my_quarter = pl.ds(pl.multiple_of(tp * quarter, LANES), quarter)
    steps = (1, -1)

    def within(at):
        return jnp.logical_and(at >= 0, at < n_rep)

    def block_rows(at, side):
        return pl.ds(pl.multiple_of((at * 2 + side) * rows, rows), rows)

    def pair_rows(at):
        return pl.ds(pl.multiple_of(at * pair, pair), pair)

    barrier = pltpu.get_barrier_semaphore()
    pl.semaphore_signal(barrier, inc=1, device_id=across, device_id_type=MESH)
    for k in range(1, n_tp):
        pl.semaphore_signal(
            barrier, inc=1, device_id={"tp": lax.rem(tp + k, n_tp)}, device_id_type=MESH
        )
    for step in steps:
        @pl.when(within(rep + step))
        def _():
            pl.semaphore_signal(
                barrier, inc=1, device_id={"rep": rep + step}, device_id_type=MESH
            )
    along = jnp.where(rep > 0, 1, 0) + jnp.where(rep < n_rep - 1, 1, 0)
    pl.semaphore_wait(barrier, n_tp + along)

    def remote(src, dst, send, recv, device):
        return pltpu.make_async_remote_copy(
            src_ref=src, dst_ref=dst, send_sem=send, recv_sem=recv,
            device_id=device, device_id_type=MESH,
        )

    def grad_across():
        src = grad_ref.at[:, pl.ds(pl.multiple_of((1 - fsdp) * half + tp * quarter, LANES), quarter)]
        return remote(src, grads.at[my_rows, my_quarter], gx_send, gx_recv, across)

    def grad_hop(i, d):
        spot = grads.at[pair_rows(rep - steps[i] * d), my_quarter]
        return remote(spot, spot, gz_send.at[i, d], gz_recv.at[i, d], {"rep": rep + steps[i]})

    def grad_arrived(i, d):
        spot = grads.at[pair_rows(rep - steps[i] * d), my_quarter]
        return remote(spot, spot, gz_send.at[i, d - 1], gz_recv.at[i, d - 1], {"rep": rep - steps[i]})

    def place(i, d):
        return 0 if d == 0 else 1 + 2 * (d - 1) + i

    def share(i, d, k, towards):
        at = rep - steps[i] * d
        peer = lax.rem(tp + (k if towards else n_tp - k), n_tp)
        source = tp if towards else peer
        cols = pl.ds(pl.multiple_of(source * quarter, LANES), quarter)
        spot = grads.at[other_rows if d == 0 else pair_rows(at), cols]
        return remote(spot, spot, gt_send.at[place(i, d), k - 1], gt_recv.at[place(i, d), k - 1], {"tp": peer})

    def hidden_hop(i, d, c):
        start, size = chunks[c]
        cols = pl.ds(start, size)
        spot = held.at[block_rows(rep - steps[i] * d, fsdp), cols]
        src = hidden_ref.at[:, cols] if d == 0 else spot
        return remote(src, spot, hz_send.at[i, d, c], hz_recv.at[i, d, c], {"rep": rep + steps[i]})

    def hidden_arrived(i, d, c):
        start, size = chunks[c]
        spot = held.at[block_rows(rep - steps[i] * d, fsdp), pl.ds(start, size)]
        return remote(spot, spot, hz_send.at[i, d - 1, c], hz_recv.at[i, d - 1, c], {"rep": rep - steps[i]})

    def hidden_across(i, d, c):
        start, size = chunks[c]
        cols = pl.ds(start, size)
        spot = held.at[block_rows(rep - steps[i] * d, fsdp), cols]
        src = hidden_ref.at[:, cols] if d == 0 else spot
        q = place(i, d)
        return remote(src, spot, hx_send.at[q, c], hx_recv.at[q, c], across)

    def hidden_crossed(i, d, c):
        start, size = chunks[c]
        spot = held.at[block_rows(rep - steps[i] * d, 1 - fsdp), pl.ds(start, size)]
        q = place(i, d)
        return remote(spot, spot, hx_send.at[q, c], hx_recv.at[q, c], across)

    def if_sends(i, act):
        pl.when(within(rep + steps[i]))(act)

    def if_meets(i, d, act):
        pl.when(within(rep - steps[i] * d))(act)

    def if_forwards(i, d, act):
        pl.when(jnp.logical_and(within(rep - steps[i] * d), within(rep + steps[i])))(act)

    count = len(chunks)
    grad_across().start()
    local_grad = pltpu.make_async_copy(
        grad_ref.at[:, pl.ds(pl.multiple_of(fsdp * half, LANES), half)], grads.at[my_rows, :], local_sem.at[0]
    )
    local_hidden = pltpu.make_async_copy(hidden_ref, held.at[my_rows, :], local_sem.at[1])
    local_grad.start()
    local_hidden.start()

    def send_own(c):
        for i in range(2):
            if_sends(i, lambda: hidden_hop(i, 0, c).start())
        hidden_across(0, 0, c).start()

    send_own(0)
    local_grad.wait()
    grad_across().wait_recv()
    for i in range(2):
        if_sends(i, lambda: grad_hop(i, 0).start())
    for k in range(1, n_tp):
        share(0, 0, k, True).start()
    for c in range(1, count):
        send_own(c)

    def take_grad(i, d):
        if_meets(i, d, lambda: grad_arrived(i, d).wait_recv())
        if d < n_rep - 1:
            if_forwards(i, d, lambda: grad_hop(i, d).start())

        def spread():
            for k in range(1, n_tp):
                share(i, d, k, True).start()
        if_meets(i, d, spread)

    def take_hidden(i, d, c):
        if_meets(i, d, lambda: hidden_arrived(i, d, c).wait_recv())
        if d < n_rep - 1:
            if_forwards(i, d, lambda: hidden_hop(i, d, c).start())
        if_meets(i, d, lambda: hidden_across(i, d, c).start())

    for d in range(1, n_rep):
        for i in range(2):
            take_grad(i, d)
        if d < n_rep - 1:
            for c in range(count):
                for i in range(2):
                    take_hidden(i, d, c)

    for k in range(1, n_tp):
        share(0, 0, k, False).wait_recv()
    for d in range(1, n_rep):
        for i in range(2):
            def wait_shared():
                for k in range(1, n_tp):
                    share(i, d, k, False).wait_recv()
            if_meets(i, d, wait_shared)
    tile = 256

    @pl.loop(0, half // tile)
    def _(m):
        spot = pl.ds(pl.multiple_of(m * tile, tile), tile)
        turned[spot, :] = grads[:, spot].T

    local_hidden.wait()
    square_ref[...] = jnp.zeros_like(square_ref)

    def out_copy(c):
        cols = pl.ds(chunks[c][0], chunks[c][1])
        return pltpu.make_async_copy(staged.at[:, cols], out_ref.at[:, cols], out_sem.at[c])

    def multiply(c):
        start, size = chunks[c]
        cols = pl.ds(start, size)
        hidden_crossed(0, 0, c).wait_recv()
        for d in range(1, n_rep):
            for i in range(2):
                if_meets(i, d, lambda: hidden_crossed(i, d, c).wait_recv())

        @pl.loop(0, half // tile)
        def _(m):
            spot = pl.ds(pl.multiple_of(m * tile, tile), tile)
            product = jnp.dot(turned[spot, :], held[:, cols], preferred_element_type=jnp.float32)
            staged[spot, cols] = product.astype(staged.dtype)
            squares = jnp.sum((product * product).reshape(tile // 8, 8, size), axis=0)
            total = squares[:, :LANES]
            for at in range(LANES, size, LANES):
                total = total + squares[:, at:at + LANES]
            square_ref[...] += total

        out_copy(c).start()

    for c in range(count):
        for i in range(2):
            take_hidden(i, n_rep - 1, c)
        if c:
            multiply(c - 1)
    multiply(count - 1)

    grad_across().wait_send()
    for k in range(1, n_tp):
        share(0, 0, k, True).wait_send()
    for i in range(2):
        def sent_own():
            grad_hop(i, 0).wait_send()
            for c in range(count):
                hidden_hop(i, 0, c).wait_send()
        if_sends(i, sent_own)
    for c in range(count):
        hidden_across(0, 0, c).wait_send()
    for d in range(1, n_rep):
        for i in range(2):
            def sent_met():
                for k in range(1, n_tp):
                    share(i, d, k, True).wait_send()
                for c in range(count):
                    hidden_across(i, d, c).wait_send()
            if_meets(i, d, sent_met)
            if d < n_rep - 1:
                def sent_on():
                    grad_hop(i, d).wait_send()
                    for c in range(count):
                        hidden_hop(i, d, c).wait_send()
                if_forwards(i, d, sent_on)
    for c in range(count):
        out_copy(c).wait()


def by_kernel(n_rep, n_tp, hidden, out_grad):
    rows, columns = hidden.shape
    tokens = rows * n_rep * 2
    half = out_grad.shape[1] // 2
    count = len(column_chunks(columns))
    dma = pltpu.SemaphoreType.DMA
    places = 1 + 2 * (n_rep - 1)
    return pl.pallas_call(
        functools.partial(gather_multiply, n_rep, n_tp),
        out_shape=(
            jax.ShapeDtypeStruct((half, columns), jnp.bfloat16),
            jax.ShapeDtypeStruct((8, LANES), jnp.float32),
        ),
        in_specs=[pl.BlockSpec(memory_space=pl.ANY)] * 2,
        out_specs=(pl.BlockSpec(memory_space=pl.ANY), pl.BlockSpec(memory_space=pltpu.VMEM)),
        scratch_shapes=[
            pltpu.VMEM((tokens, columns), jnp.bfloat16),
            pltpu.VMEM((tokens, half), jnp.bfloat16),
            pltpu.VMEM((half, tokens), jnp.bfloat16),
            pltpu.VMEM((half, columns), jnp.bfloat16),
            dma((2,)), dma, dma,
            dma((2, n_rep - 1)), dma((2, n_rep - 1)),
            dma((places, n_tp - 1)), dma((places, n_tp - 1)),
            dma((2, n_rep - 1, count)), dma((2, n_rep - 1, count)),
            dma((places, count)), dma((places, count)),
            dma((count,)),
        ],
        compiler_params=pltpu.CompilerParams(
            collective_id=0, has_side_effects=True, vmem_limit_bytes=VMEM_LIMIT
        ),
    )(hidden, out_grad)


def by_xla(hidden, out_grad):
    spread = lax.all_to_all(out_grad, "fsdp", split_axis=1, concat_axis=0, tiled=True)
    grad_rows = lax.all_gather(spread, "rep", axis=0, tiled=True)
    hidden_rows = lax.all_gather(hidden, ("rep", "fsdp"), axis=0, tiled=True)
    summed = lax.dot_general(
        grad_rows, hidden_rows, (((0,), (0,)), ((), ())), preferred_element_type=jnp.float32
    )
    return summed, jnp.sum(summed * summed)


def kernel_fits(n_rep, n_fsdp, n_tp, rows, columns, features):
    tokens, half = rows * n_rep * n_fsdp, features // n_fsdp
    held_bytes = 2 * (tokens * columns + 2 * tokens * half + half * columns)
    aligned = rows % 16 == 0 and columns % LANES == 0 and half % (LANES * n_tp) == 0
    return n_fsdp == 2 and aligned and half % 256 == 0 and held_bytes < VMEM_LIMIT * 3 // 4


def solution(mesh):
    n_rep, n_fsdp, n_tp = (mesh.shape[axis] for axis in ("rep", "fsdp", "tp"))

    def on_device(gate_pre, up_pre, out_grad):
        hidden = (jax.nn.silu(gate_pre.astype(jnp.float32)) * up_pre.astype(jnp.float32)).astype(
            jnp.bfloat16
        )
        if kernel_fits(n_rep, n_fsdp, n_tp, *hidden.shape, out_grad.shape[1]):
            summed, squares = by_kernel(n_rep, n_tp, hidden, out_grad)
            square_sum = jnp.sum(squares)
        else:
            summed, square_sum = by_xla(hidden, out_grad)
        square_total = lax.psum(square_sum, ("fsdp", "tp"))
        entry_count = summed.shape[0] * n_fsdp * summed.shape[1] * n_tp
        factor = 1.0 / jnp.sqrt(square_total / entry_count + 1e-06)
        return (summed.astype(jnp.float32) * factor).astype(jnp.bfloat16)

    return jax.shard_map(
        on_device,
        mesh=mesh,
        in_specs=(P(("rep", "fsdp"), "tp"), P(("rep", "fsdp"), "tp"), P(("rep", "fsdp"), None)),
        out_specs=P("fsdp", "tp"),
        check_vma=False,
    )
```

```python
import functools

import jax
import jax.numpy as jnp
from jax import lax
from jax.experimental import pallas as pl
from jax.experimental.pallas import tpu as pltpu
from jax.sharding import PartitionSpec as P

MESH = pl.DeviceIdType.MESH
LANES = 128
VMEM_LIMIT = 60 * 1024 * 1024


def column_chunks(columns):
    chunks, start = [], 0
    for tiles in (6, 4, 2, 1):
        while columns - start >= tiles * LANES:
            chunks.append((start, tiles * LANES))
            start += tiles * LANES
    return chunks


def gather_multiply(
    n_rep, n_tp, entry_count, hidden_ref, grad_ref, out_ref, factor_ref,
    held, grads, turned, sums,
    local_sem, gx_send, gx_recv, gz_send, gz_recv, gt_send, gt_recv,
    hz_send, hz_recv, hx_send, hx_recv, sq_send, sq_recv,
):
    rep = lax.axis_index("rep")
    fsdp = lax.axis_index("fsdp")
    tp = lax.axis_index("tp")
    rows, columns = hidden_ref.shape
    half = grads.shape[1]
    quarter = half // n_tp
    chunks = column_chunks(columns)
    pair = 2 * rows
    my_slot = rep * 2 + fsdp
    my_rows = pl.ds(pl.multiple_of(my_slot * rows, rows), rows)
    other_rows = pl.ds(pl.multiple_of((rep * 2 + 1 - fsdp) * rows, rows), rows)
    across = {"fsdp": 1 - fsdp}
    my_quarter = pl.ds(pl.multiple_of(tp * quarter, LANES), quarter)
    steps = (1, -1)

    def within(at):
        return jnp.logical_and(at >= 0, at < n_rep)

    def block_rows(at, side):
        return pl.ds(pl.multiple_of((at * 2 + side) * rows, rows), rows)

    def pair_rows(at):
        return pl.ds(pl.multiple_of(at * pair, pair), pair)

    barrier = pltpu.get_barrier_semaphore()
    pl.semaphore_signal(barrier, inc=1, device_id=across, device_id_type=MESH)
    for k in range(1, n_tp):
        pl.semaphore_signal(
            barrier, inc=1, device_id={"tp": lax.rem(tp + k, n_tp)}, device_id_type=MESH
        )
        pl.semaphore_signal(
            barrier, inc=1, device_id={"fsdp": 1 - fsdp, "tp": lax.rem(tp + k, n_tp)},
            device_id_type=MESH,
        )
    for step in steps:
        @pl.when(within(rep + step))
        def _():
            pl.semaphore_signal(
                barrier, inc=1, device_id={"rep": rep + step}, device_id_type=MESH
            )
    along = jnp.where(rep > 0, 1, 0) + jnp.where(rep < n_rep - 1, 1, 0)
    pl.semaphore_wait(barrier, 2 * n_tp - 1 + along)

    def remote(src, dst, send, recv, device):
        return pltpu.make_async_remote_copy(
            src_ref=src, dst_ref=dst, send_sem=send, recv_sem=recv,
            device_id=device, device_id_type=MESH,
        )

    def grad_across():
        src = grad_ref.at[:, pl.ds(pl.multiple_of((1 - fsdp) * half + tp * quarter, LANES), quarter)]
        return remote(src, grads.at[my_rows, my_quarter], gx_send, gx_recv, across)

    def grad_hop(i, d):
        spot = grads.at[pair_rows(rep - steps[i] * d), my_quarter]
        return remote(spot, spot, gz_send.at[i, d], gz_recv.at[i, d], {"rep": rep + steps[i]})

    def grad_arrived(i, d):
        spot = grads.at[pair_rows(rep - steps[i] * d), my_quarter]
        return remote(spot, spot, gz_send.at[i, d - 1], gz_recv.at[i, d - 1], {"rep": rep - steps[i]})

    def place(i, d):
        return 0 if d == 0 else 1 + 2 * (d - 1) + i

    def share(i, d, k, towards):
        at = rep - steps[i] * d
        peer = lax.rem(tp + (k if towards else n_tp - k), n_tp)
        source = tp if towards else peer
        cols = pl.ds(pl.multiple_of(source * quarter, LANES), quarter)
        spot = grads.at[other_rows if d == 0 else pair_rows(at), cols]
        return remote(spot, spot, gt_send.at[place(i, d), k - 1], gt_recv.at[place(i, d), k - 1], {"tp": peer})

    def hidden_hop(i, d, c):
        start, size = chunks[c]
        cols = pl.ds(start, size)
        spot = held.at[block_rows(rep - steps[i] * d, fsdp), cols]
        src = hidden_ref.at[:, cols] if d == 0 else spot
        return remote(src, spot, hz_send.at[i, d, c], hz_recv.at[i, d, c], {"rep": rep + steps[i]})

    def hidden_arrived(i, d, c):
        start, size = chunks[c]
        spot = held.at[block_rows(rep - steps[i] * d, fsdp), pl.ds(start, size)]
        return remote(spot, spot, hz_send.at[i, d - 1, c], hz_recv.at[i, d - 1, c], {"rep": rep - steps[i]})

    def hidden_across(i, d, c):
        start, size = chunks[c]
        cols = pl.ds(start, size)
        spot = held.at[block_rows(rep - steps[i] * d, fsdp), cols]
        src = hidden_ref.at[:, cols] if d == 0 else spot
        q = place(i, d)
        return remote(src, spot, hx_send.at[q, c], hx_recv.at[q, c], across)

    def hidden_crossed(i, d, c):
        start, size = chunks[c]
        spot = held.at[block_rows(rep - steps[i] * d, 1 - fsdp), pl.ds(start, size)]
        q = place(i, d)
        return remote(spot, spot, hx_send.at[q, c], hx_recv.at[q, c], across)

    def if_sends(i, act):
        pl.when(within(rep + steps[i]))(act)

    def if_meets(i, d, act):
        pl.when(within(rep - steps[i] * d))(act)

    def if_forwards(i, d, act):
        pl.when(jnp.logical_and(within(rep - steps[i] * d), within(rep + steps[i])))(act)

    count = len(chunks)
    grad_across().start()
    local_grad = pltpu.make_async_copy(
        grad_ref.at[:, pl.ds(pl.multiple_of(fsdp * half, LANES), half)], grads.at[my_rows, :], local_sem.at[0]
    )
    local_hidden = pltpu.make_async_copy(hidden_ref, held.at[my_rows, :], local_sem.at[1])
    local_grad.start()
    local_hidden.start()

    def send_own(c):
        for i in range(2):
            if_sends(i, lambda: hidden_hop(i, 0, c).start())
        hidden_across(0, 0, c).start()

    send_own(0)
    local_grad.wait()
    grad_across().wait_recv()
    for i in range(2):
        if_sends(i, lambda: grad_hop(i, 0).start())
    for k in range(1, n_tp):
        share(0, 0, k, True).start()
    for c in range(1, count):
        send_own(c)

    def take_grad(i, d):
        if_meets(i, d, lambda: grad_arrived(i, d).wait_recv())
        if d < n_rep - 1:
            if_forwards(i, d, lambda: grad_hop(i, d).start())

        def spread():
            for k in range(1, n_tp):
                share(i, d, k, True).start()
        if_meets(i, d, spread)

    def take_hidden(i, d, c):
        if_meets(i, d, lambda: hidden_arrived(i, d, c).wait_recv())
        if d < n_rep - 1:
            if_forwards(i, d, lambda: hidden_hop(i, d, c).start())
        if_meets(i, d, lambda: hidden_across(i, d, c).start())

    for d in range(1, n_rep):
        for i in range(2):
            take_grad(i, d)
        if d < n_rep - 1:
            for c in range(count):
                for i in range(2):
                    take_hidden(i, d, c)

    for k in range(1, n_tp):
        share(0, 0, k, False).wait_recv()
    for d in range(1, n_rep):
        for i in range(2):
            def wait_shared():
                for k in range(1, n_tp):
                    share(i, d, k, False).wait_recv()
            if_meets(i, d, wait_shared)
    tile = 256

    @pl.loop(0, half // tile)
    def _(m):
        spot = pl.ds(pl.multiple_of(m * tile, tile), tile)
        turned[spot, :] = grads[:, spot].T

    local_hidden.wait()
    mine = fsdp * n_tp + tp
    sums[mine] = jnp.zeros(sums.shape[1:], sums.dtype)

    def multiply(c):
        start, size = chunks[c]
        cols = pl.ds(start, size)
        hidden_crossed(0, 0, c).wait_recv()
        for d in range(1, n_rep):
            for i in range(2):
                if_meets(i, d, lambda: hidden_crossed(i, d, c).wait_recv())

        @pl.loop(0, half // tile)
        def _(m):
            spot = pl.ds(pl.multiple_of(m * tile, tile), tile)
            product = jnp.dot(turned[spot, :], held[:, cols], preferred_element_type=jnp.float32)
            out_ref[spot, cols] = product.astype(out_ref.dtype)
            squares = jnp.sum((product * product).reshape(tile // 8, 8, size), axis=0)
            total = squares[:, :LANES]
            for at in range(LANES, size, LANES):
                total = total + squares[:, at:at + LANES]
            sums[mine] += total

    for c in range(count):
        for i in range(2):
            take_hidden(i, n_rep - 1, c)
        if c:
            multiply(c - 1)
    multiply(count - 1)

    grad_across().wait_send()
    for k in range(1, n_tp):
        share(0, 0, k, True).wait_send()
    for i in range(2):
        def sent_own():
            grad_hop(i, 0).wait_send()
            for c in range(count):
                hidden_hop(i, 0, c).wait_send()
        if_sends(i, sent_own)
    for c in range(count):
        hidden_across(0, 0, c).wait_send()
    for d in range(1, n_rep):
        for i in range(2):
            def sent_met():
                for k in range(1, n_tp):
                    share(i, d, k, True).wait_send()
                for c in range(count):
                    hidden_across(i, d, c).wait_send()
            if_meets(i, d, sent_met)
            if d < n_rep - 1:
                def sent_on():
                    grad_hop(i, d).wait_send()
                    for c in range(count):
                        hidden_hop(i, d, c).wait_send()
                if_forwards(i, d, sent_on)

    peers = [(across_k, k) for across_k in range(2) for k in range(n_tp) if across_k or k]

    def exchange(at, towards):
        side, k = peers[at]
        to_side = 1 - fsdp if side else fsdp
        to_tp = lax.rem(tp + (k if towards else n_tp - k), n_tp)
        spot = sums.at[mine if towards else to_side * n_tp + to_tp]
        return remote(spot, spot, sq_send.at[at], sq_recv.at[at], {"fsdp": to_side, "tp": to_tp})

    for at in range(len(peers)):
        exchange(at, True).start()
    for at in range(len(peers)):
        exchange(at, False).wait_recv()
    square_total = jnp.sum(jnp.sum(sums[...], axis=0), keepdims=True)
    factor = 1.0 / jnp.sqrt(square_total / entry_count + 1e-06)
    factor_ref[...] = jnp.broadcast_to(factor, factor_ref.shape)
    for at in range(len(peers)):
        exchange(at, True).wait_send()


def by_kernel(n_rep, n_tp, entry_count, hidden, out_grad):
    rows, columns = hidden.shape
    tokens = rows * n_rep * 2
    half = out_grad.shape[1] // 2
    count = len(column_chunks(columns))
    dma = pltpu.SemaphoreType.DMA
    places = 1 + 2 * (n_rep - 1)
    return pl.pallas_call(
        functools.partial(gather_multiply, n_rep, n_tp, entry_count),
        out_shape=(
            pltpu.VMEM((half, columns), jnp.bfloat16),
            pltpu.VMEM((8, LANES), jnp.float32),
        ),
        in_specs=[pl.BlockSpec(memory_space=pl.ANY)] * 2,
        out_specs=(pl.BlockSpec(memory_space=pltpu.VMEM), pl.BlockSpec(memory_space=pltpu.VMEM)),
        scratch_shapes=[
            pltpu.VMEM((tokens, columns), jnp.bfloat16),
            pltpu.VMEM((tokens, half), jnp.bfloat16),
            pltpu.VMEM((half, tokens), jnp.bfloat16),
            pltpu.VMEM((2 * n_tp, 8, LANES), jnp.float32),
            dma((2,)), dma, dma,
            dma((2, n_rep - 1)), dma((2, n_rep - 1)),
            dma((places, n_tp - 1)), dma((places, n_tp - 1)),
            dma((2, n_rep - 1, count)), dma((2, n_rep - 1, count)),
            dma((places, count)), dma((places, count)),
            dma((2 * n_tp - 1,)), dma((2 * n_tp - 1,)),
        ],
        compiler_params=pltpu.CompilerParams(
            collective_id=0, has_side_effects=True, vmem_limit_bytes=VMEM_LIMIT * 2 // 3
        ),
    )(hidden, out_grad)


def scale(summed, factors):
    half, columns = summed.shape
    rows = 128

    def body(summed_ref, factor_ref, out_ref, ready, sems):
        steps = half // rows
        depth = ready.shape[0]

        def leave(m):
            slot = lax.rem(m, depth)
            spot = pl.ds(pl.multiple_of(m * rows, rows), rows)
            return pltpu.make_async_copy(ready.at[slot], out_ref.at[spot, :], sems.at[slot])

        @pl.loop(0, steps)
        def _(m):
            slot = lax.rem(m, depth)
            spot = pl.ds(pl.multiple_of(m * rows, rows), rows)

            @pl.when(m >= depth)
            def _():
                leave(m - depth).wait()
            for at in range(0, columns, LANES):
                cols = pl.ds(at, LANES)
                scaled = summed_ref[spot, cols].astype(jnp.float32) * factor_ref[0:1, :]
                ready[slot, :, cols] = scaled.astype(ready.dtype)
            leave(m).start()

        @pl.loop(max(steps - depth, 0), steps)
        def _(m):
            leave(m).wait()

    return pl.pallas_call(
        body,
        out_shape=jax.ShapeDtypeStruct((half, columns), jnp.bfloat16),
        in_specs=[pl.BlockSpec(memory_space=pltpu.VMEM)] * 2,
        out_specs=pl.BlockSpec(memory_space=pl.ANY),
        scratch_shapes=[pltpu.VMEM((4, rows, columns), jnp.bfloat16), pltpu.SemaphoreType.DMA((4,))],
        compiler_params=pltpu.CompilerParams(vmem_limit_bytes=16 * 1024 * 1024),
    )(summed, factors)


def by_xla(hidden, out_grad):
    spread = lax.all_to_all(out_grad, "fsdp", split_axis=1, concat_axis=0, tiled=True)
    grad_rows = lax.all_gather(spread, "rep", axis=0, tiled=True)
    hidden_rows = lax.all_gather(hidden, ("rep", "fsdp"), axis=0, tiled=True)
    summed = lax.dot_general(
        grad_rows, hidden_rows, (((0,), (0,)), ((), ())), preferred_element_type=jnp.float32
    )
    return summed, jnp.sum(summed * summed)


def kernel_fits(n_rep, n_fsdp, n_tp, rows, columns, features):
    tokens, half = rows * n_rep * n_fsdp, features // n_fsdp
    held_bytes = 2 * (tokens * columns + 2 * tokens * half + half * columns)
    aligned = rows % 16 == 0 and columns % LANES == 0 and half % (LANES * n_tp) == 0
    return n_fsdp == 2 and aligned and half % 256 == 0 and held_bytes < VMEM_LIMIT * 3 // 4


def solution(mesh):
    n_rep, n_fsdp, n_tp = (mesh.shape[axis] for axis in ("rep", "fsdp", "tp"))

    def on_device(gate_pre, up_pre, out_grad):
        hidden = (jax.nn.silu(gate_pre.astype(jnp.float32)) * up_pre.astype(jnp.float32)).astype(
            jnp.bfloat16
        )
        half, columns = out_grad.shape[1] // n_fsdp, hidden.shape[1]
        entry_count = half * n_fsdp * columns * n_tp
        if kernel_fits(n_rep, n_fsdp, n_tp, *hidden.shape, out_grad.shape[1]):
            summed, factors = by_kernel(n_rep, n_tp, entry_count, hidden, out_grad)
            return scale(summed, factors)
        summed, square_sum = by_xla(hidden, out_grad)
        square_total = lax.psum(square_sum, ("fsdp", "tp"))
        factor = 1.0 / jnp.sqrt(square_total / entry_count + 1e-06)
        return (summed * factor).astype(jnp.bfloat16)

    return jax.shard_map(
        on_device,
        mesh=mesh,
        in_specs=(P(("rep", "fsdp"), "tp"), P(("rep", "fsdp"), "tp"), P(("rep", "fsdp"), None)),
        out_specs=P("fsdp", "tp"),
        check_vma=False,
    )
```
